32 devices in a mesh: dp: 4 (over z), seq: 2 (over x), tensor: 4 (over y, core).
Axes of the slice: x: 2, y: 2, z: 4, core: 2. Of those that a mesh axis runs over, the one named last changes fastest.
Arguments:
- hidden_in: bfloat16 [16384, 2880], P(('dp', 'seq', 'tensor')), parts along dimension 0, may hold values from -6 to 6
- norm_gain: float32 [2880], replicated, may hold values from 0.5 to 1.5
- conv_weight: float32 [4, 2880], replicated, may hold values from -3 to 3
- w_query: bfloat16 [2880, 2048], P(None, 'tensor'), may hold values from -32 to 32
- w_key: bfloat16 [2880, 512], P(None, 'tensor'), may hold values from -1 to 1
- w_value: bfloat16 [2880, 512], P(None, 'tensor'), may hold values from -0.109375 to 0.109375
- w_out: bfloat16 [2048, 2880], P('tensor'), may hold values from -0.125 to 0.125
- doc_ids: int32 [16384], P(('dp', 'seq')), parts along dimension 0, may hold values from 0 to 15, never falling along the last dimension, each value on 1 to 1024 neighbouring positions
Outputs:
- hidden_out: bfloat16 [16384, 2880], P(('dp', 'seq', 'tensor')), parts along dimension 0
The draws below stay inside these ranges and needn't reach their ends.
There are 4 independent parts, one for each index of `dp`. The reference program is written for one: setup_inputs(seed, part) draws one part's arguments, and reference() takes and returns one part's arrays. A program takes and returns all parts, laid end to end along the dimension named above; an argument that names none is the same for every part. Nothing has to cross between parts.
Inputs may be any that keep to these rules, and one draw needn't show every extreme that they name: `doc_ids`: document numbers never fall along a window's tokens.
All inputs are finite; a program needn't handle non-finite values.
Results may differ from the reference program's by a relative error of at most 0.011.
Values may be sent and summed in bfloat16 or wider, within the bound.
No kernel may reach another device: no remote copies, remote signals or barrier semaphores. Data moves between devices by JAX's collectives and lax.ppermute only.
A program may use at most 128 MiB of HBM per device.

```python
import math
import jax
import jax.numpy as jnp
import numpy as np
from jax import lax

D = 2880
HEADS = 32
KV_HEADS = 8
HEAD = 64
KERNEL = 4
WINDOW = 128
QBLOCK = 512
TOKENS = 4096
DOC_MOST = 1024
DOCS = 16


def key_matrix(key):
    scale = 1.0 / math.sqrt(D)
    raw = jax.random.normal(jax.random.fold_in(key, 11), (D, KV_HEADS * HEAD), jnp.float32) * scale
    return jnp.clip(raw, -5.0 * scale, 5.0 * scale)


def draw_w_key(key, part):
    return key_matrix(key).astype(jnp.bfloat16)


def draw_w_query(key, part):
    noise = jax.random.normal(jax.random.fold_in(key, 13), (D, HEADS * HEAD), jnp.float32) * (1.0 / math.sqrt(D))
    return noise.astype(jnp.bfloat16)


def steps_of(rng, shape, pieces, least, high):
    level = 1.0
    for dim, blocks in pieces:
        draws = jax.random.uniform(jax.random.fold_in(jax.random.fold_in(rng, 6), dim), (blocks,), jnp.float32, least / len(pieces), high / len(pieces))
        level = level * jnp.repeat(jnp.exp(draws), shape[dim] // blocks).reshape((-1,) + (1,) * (len(shape) - 1 - dim))
    return level


def length_profile(number_of, total, reach, lean):
    loads = [(1 << 20) // math.isqrt(grade ** lean) + 1 for grade in range(2, number_of + 1)]
    surplus, given = total - reach - (number_of - 1), [1] * (number_of - 1)
    while surplus > 0:
        movable = [i for i in range(number_of - 1) if given[i] < reach]
        pool, left = sum([loads[i] for i in movable]), surplus
        for i in movable:
            addition = min(reach - given[i], max(1, left * loads[i] // pool), surplus)
            given[i] = given[i] + addition
            surplus = surplus - addition
    return np.array([reach] + given)


def uneven_parts(own_key, amount, total, reach, slope):
    if amount == 2:
        one = jax.random.randint(own_key, (), max(1, total - reach), min(reach, total - 1) + 1)
        return jnp.stack([one, total - one])
    lengths = jnp.asarray(length_profile(amount, total, reach, slope), jnp.int32)
    pairs = (amount - 1) // 2
    donor, sink = lengths[1:1 + 2 * pairs:2], lengths[2:2 + 2 * pairs:2]
    slack = jnp.minimum(donor - 1, reach - sink)
    moved = jax.random.randint(jax.random.fold_in(own_key, 1), (pairs,), 0, 1 << 20) % (slack + 1)
    lengths = lengths.at[1:1 + 2 * pairs:2].set(donor - moved).at[2:2 + 2 * pairs:2].set(sink + moved)
    return lengths[jax.random.permutation(jax.random.fold_in(own_key, 2), amount)]


def normal_values(stream_key, extent, deviation, most, split=(), kind=jnp.bfloat16):
    loudness = steps_of(stream_key, extent, split, -0.22, 0.18) if split else 1.0
    values = jax.random.normal(stream_key, extent, jnp.float32) * deviation * loudness
    return jnp.minimum(jnp.maximum(values, -most), most).astype(kind)


def setup_inputs(seed: int = 0, part: int = 0) -> dict:
    arg_keys = jax.random.split(jax.random.key(seed), 9)
    part_keys = jax.random.split(jax.random.fold_in(arg_keys[8], part), 9)
    return {
        "hidden_in": normal_values(part_keys[0], (TOKENS, D), 1.0, 6.0, ((0, 8),)),
        "norm_gain": jnp.clip(1.0 + 0.1 * jax.random.normal(arg_keys[1], (D,), jnp.float32), 0.5, 1.5),
        "conv_weight": normal_values(arg_keys[2], (KERNEL, D), 0.5, 3.0, (), jnp.float32),
        "w_query": draw_w_query(jax.random.fold_in(arg_keys[8], 71), part),
        "w_key": draw_w_key(jax.random.fold_in(arg_keys[8], 71), part),
        "w_value": normal_values(arg_keys[5], (D, KV_HEADS * HEAD), D ** -0.5, 0.109375, ((1, 4),)),
        "w_out": normal_values(arg_keys[6], (HEADS * HEAD, D), (HEADS * HEAD) ** -0.5, 0.125, ((0, 4),)),
        "doc_ids": jnp.searchsorted(jnp.cumsum(uneven_parts(part_keys[7], DOCS, TOKENS, DOC_MOST, 2)), jnp.arange(TOKENS), side="right").astype(jnp.int32),
    }


eps = 1e-05
rope_base = 150000.0

def rotate(values, positions):
    rows = values.shape[0]
    half = HEAD // 2
    frequency = jnp.exp(jnp.arange(half, dtype=jnp.float32) * (-2.0 * math.log(rope_base) / HEAD))
    angle = positions.astype(jnp.float32)[:, None] * frequency[None, :]
    cosine = jnp.cos(angle)[:, None, :]
    sine = jnp.sin(angle)[:, None, :]
    shaped = values.reshape(rows, -1, HEAD)
    first = shaped[:, :, :half]
    second = shaped[:, :, half:]
    turned = jnp.concatenate([first * cosine - second * sine, second * cosine + first * sine], axis=2)
    return turned.reshape(rows, -1)

def attend(queries, keys, values, query_pos, key_pos, query_doc, key_doc):
    scores = jnp.einsum('qhgd,khd->hgqk', queries.astype(jnp.float32), keys.astype(jnp.float32)) * (1.0 / math.sqrt(HEAD))
    visible = (key_pos[None, :] <= query_pos[:, None]) & (key_pos[None, :] > query_pos[:, None] - WINDOW)
    visible = visible & (key_pos[None, :] >= 0) & (key_doc[None, :] == query_doc[:, None])
    scores = jnp.where(visible[None, None, :, :], scores, -jnp.inf)
    largest = lax.optimization_barrier(jnp.max(scores, axis=3, keepdims=True))
    weights = jnp.exp(scores - largest)
    total = lax.optimization_barrier(jnp.sum(weights, axis=3))
    rounded = weights.astype(jnp.bfloat16)
    summed = jnp.einsum('hgqk,khd->qhgd', rounded.astype(jnp.float32), values.astype(jnp.float32))
    result = summed / jnp.transpose(total, (2, 0, 1))[:, :, :, None]
    return result.reshape(result.shape[0], -1).astype(jnp.bfloat16)

def reference(hidden_in, norm_gain, conv_weight, w_query, w_key, w_value, w_out, doc_ids):
    total_rows = hidden_in.shape[0]
    inputs = hidden_in.astype(jnp.float32)
    mean_square = lax.optimization_barrier(jnp.mean(inputs * inputs, axis=1, keepdims=True))
    normed = (inputs * lax.rsqrt(mean_square + eps) * norm_gain[None, :]).astype(jnp.bfloat16)
    padded = jnp.concatenate([jnp.zeros((KERNEL - 1, D), jnp.float32), normed.astype(jnp.float32)], axis=0)
    convolved = jnp.zeros((total_rows, D), jnp.float32)
    for tap in range(KERNEL):
        convolved = convolved + conv_weight[tap][None, :] * padded[KERNEL - 1 - tap:KERNEL - 1 - tap + total_rows]
    mixed = convolved.astype(jnp.bfloat16)
    positions = jnp.arange(total_rows, dtype=jnp.int32)
    queries = rotate(jnp.dot(mixed, w_query, preferred_element_type=jnp.float32), positions).astype(jnp.bfloat16)
    keys = rotate(jnp.dot(mixed, w_key, preferred_element_type=jnp.float32), positions).astype(jnp.bfloat16)
    values = jnp.dot(mixed, w_value, preferred_element_type=jnp.float32).astype(jnp.bfloat16)
    groups = HEADS // KV_HEADS
    query_four = queries.reshape(total_rows, KV_HEADS, groups, HEAD)
    key_pad = jnp.concatenate([jnp.zeros((WINDOW, KV_HEADS * HEAD), jnp.bfloat16), keys], axis=0).reshape(total_rows + WINDOW, KV_HEADS, HEAD)
    value_pad = jnp.concatenate([jnp.zeros((WINDOW, KV_HEADS * HEAD), jnp.bfloat16), values], axis=0).reshape(total_rows + WINDOW, KV_HEADS, HEAD)
    doc_pad = jnp.concatenate([jnp.full((WINDOW,), -1, jnp.int32), doc_ids.astype(jnp.int32)], axis=0)
    pos_pad = jnp.arange(total_rows + WINDOW, dtype=jnp.int32) - WINDOW

    def one_block(index):
        begin = (index * QBLOCK).astype(jnp.int32)
        block_q = lax.dynamic_slice_in_dim(query_four, begin, QBLOCK, 0)
        block_k = lax.dynamic_slice_in_dim(key_pad, begin, QBLOCK + WINDOW, 0)
        block_v = lax.dynamic_slice_in_dim(value_pad, begin, QBLOCK + WINDOW, 0)
        query_pos = lax.dynamic_slice_in_dim(positions, begin, QBLOCK, 0)
        key_pos = lax.dynamic_slice_in_dim(pos_pad, begin, QBLOCK + WINDOW, 0)
        query_doc = lax.dynamic_slice_in_dim(doc_ids.astype(jnp.int32), begin, QBLOCK, 0)
        key_doc = lax.dynamic_slice_in_dim(doc_pad, begin, QBLOCK + WINDOW, 0)
        return attend(block_q, block_k, block_v, query_pos, key_pos, query_doc, key_doc)
    blocks = lax.map(one_block, jnp.arange(total_rows // QBLOCK, dtype=jnp.int32))
    attended = blocks.reshape(total_rows, HEADS * HEAD)
    projected = jnp.dot(attended, w_out, preferred_element_type=jnp.float32)
    return (inputs + projected).astype(jnp.bfloat16)
```

```python
import math

import jax
import jax.numpy as jnp
from jax import lax
from jax.experimental import pallas as pl
from jax.experimental.pallas import tpu as pltpu
from jax.sharding import PartitionSpec as P

HEAD = 64
WINDOW = 128
LANES = 128

eps = 1e-05
rope_base = 150000.0


def swapped(array, axis, bit):
    devices = lax.axis_size(axis)
    return lax.ppermute(array, axis, [(i, i ^ bit) for i in range(devices)])


def tables(rows, start):
    half = HEAD // 2
    frequency = jnp.exp(jnp.arange(half, dtype=jnp.float32) * (-2.0 * math.log(rope_base) / HEAD))
    positions = start + jnp.arange(rows, dtype=jnp.int32)
    angle = positions.astype(jnp.float32)[:, None] * frequency[None, :]
    cosine = jnp.cos(angle)
    sine = jnp.sin(angle)
    return (
        jnp.concatenate([cosine] * (LANES // half), axis=1),
        jnp.concatenate([-sine, sine] * (LANES // HEAD), axis=1),
    )


def attention_kernel(query_cols, key_cols, proj, cosine, sine, query_doc, key_doc, out):
    span = out.shape[0]
    half = HEAD // 2
    groups = query_cols // key_cols
    lane = lax.broadcasted_iota(jnp.int32, (1, LANES), 1)
    low = (lane % HEAD) < half

    def turn(values, cos, sin):
        other = jnp.where(low, pltpu.roll(values, LANES - half, 1), pltpu.roll(values, half, 1))
        return values * cos + other * sin

    keys = []
    for c in range(key_cols // LANES):
        at = query_cols + c * LANES
        keys.append(turn(proj[:, at : at + LANES], cosine[:, :], sine[:, :]).astype(jnp.bfloat16))
    first = query_cols + key_cols
    values = proj[:, first : first + key_cols].astype(jnp.bfloat16)
    row = lax.broadcasted_iota(jnp.int32, (WINDOW, 2 * WINDOW), 0)
    col = lax.broadcasted_iota(jnp.int32, (WINDOW, 2 * WINDOW), 1)
    band = (col > row) & (col <= row + WINDOW)
    for block in range(span // WINDOW):
        q0 = block * WINDOW
        cos = cosine[q0 + WINDOW : q0 + 2 * WINDOW, :]
        sin = sine[q0 + WINDOW : q0 + 2 * WINDOW, :]
        same = query_doc[q0 : q0 + WINDOW, :] == key_doc[:, q0 : q0 + 2 * WINDOW]
        visible = band & same
        mask = jnp.concatenate([visible] * groups, axis=0)
        for kv in range(key_cols // HEAD):
            heads = []
            for c in range(groups * HEAD // LANES):
                at = kv * groups * HEAD + c * LANES
                turned = turn(proj[q0 + WINDOW : q0 + 2 * WINDOW, at : at + LANES], cos, sin)
                turned = (turned * (1.0 / math.sqrt(HEAD))).astype(jnp.bfloat16)
                for h in range(LANES // HEAD):
                    heads.append(turned[:, h * HEAD : (h + 1) * HEAD])
            stacked = jnp.concatenate(heads, axis=0)
            lo = (kv * HEAD) % LANES
            key = keys[kv * HEAD // LANES][q0 : q0 + 2 * WINDOW, lo : lo + HEAD]
            value = values[q0 : q0 + 2 * WINDOW, kv * HEAD : (kv + 1) * HEAD]
            scores = lax.dot_general(
                stacked, key, (((1,), (1,)), ((), ())), preferred_element_type=jnp.float32
            )
            scores = jnp.where(mask, scores, -1e30)
            largest = jnp.max(scores, axis=1, keepdims=True)
            weights = jnp.exp(scores - largest)
            total = jnp.sum(weights, axis=1, keepdims=True)
            summed = jnp.dot(
                weights.astype(jnp.bfloat16), value, preferred_element_type=jnp.float32
            )
            result = (summed / total).astype(jnp.bfloat16)
            pieces = [result[g * WINDOW : (g + 1) * WINDOW, :] for g in range(groups)]
            at = kv * groups * HEAD
            out[q0 : q0 + WINDOW, at : at + groups * HEAD] = jnp.concatenate(pieces, axis=1)


def attention(proj, cosine, sine, query_doc, key_doc, query_cols, key_cols):
    rows = query_doc.shape[0]

    def kernel(*refs):
        attention_kernel(query_cols, key_cols, *refs)

    return pl.pallas_call(
        kernel,
        out_shape=jax.ShapeDtypeStruct((rows, query_cols), jnp.bfloat16),
        cost_estimate=pl.CostEstimate(
            flops=rows * query_cols * 2 * WINDOW * 4,
            bytes_accessed=proj.size * 4,
            transcendentals=rows * query_cols // HEAD * 2 * WINDOW,
        ),
        name="attention",
    )(proj, cosine, sine, query_doc, key_doc)


def product(left, right):
    return jnp.dot(left, right, preferred_element_type=jnp.float32)


def local(hidden_in, norm_gain, conv_weight, w_query, w_key, w_value, w_out, doc_ids):
    rows, width = hidden_in.shape
    taps = conv_weight.shape[0]
    query_cols = w_query.shape[1]
    key_cols = w_key.shape[1]
    tensors = lax.axis_size("tensor")
    part = lax.axis_index("tensor")
    line = lax.axis_index("seq") * tensors + part
    far = tensors // 2
    place = 2 * (lax.axis_index("seq") % 2) + lax.axis_index("dp") % 2
    quarter = width // 4
    out_quarter = query_cols // 4

    def qkv_piece(which):
        at = which * quarter
        return jnp.concatenate(
            [lax.dynamic_slice_in_dim(w, at, quarter, 0) for w in (w_query, w_key, w_value)], axis=1
        )

    def out_piece(which):
        return lax.dynamic_slice_in_dim(w_out, which * out_quarter, out_quarter, 0)

    def fetched(piece, gate):
        first_piece = piece(place)
        if gate is not None:
            first_piece, _ = lax.optimization_barrier((first_piece, gate))
        zero = swapped(first_piece, "tensor", far)
        last_piece, zero = lax.optimization_barrier((piece(place ^ 3), zero))
        three = swapped(last_piece, "tensor", far)
        one = swapped(zero, "dp", 1)
        two = swapped(zero, "seq", 1)
        return [zero, one, two, three]

    qkv_far = fetched(qkv_piece, None)
    out_far = fetched(out_piece, qkv_far[3][:8, :LANES])

    lead = WINDOW + 16
    own_doc = lax.dynamic_slice_in_dim(doc_ids, part * rows, rows, 0)
    sent = jnp.concatenate(
        [
            hidden_in[rows - lead :],
            jnp.broadcast_to(
                own_doc[rows - lead :].astype(jnp.bfloat16)[:, None], (lead, LANES)
            ),
        ],
        axis=1,
    )
    devices = lax.axis_size("seq") * tensors
    rim = lax.ppermute(sent, ("seq", "tensor"), [(i, i + 1) for i in range(devices - 1)])
    rim_doc = jnp.where(line == 0, -1, rim[lead - WINDOW :, width].astype(jnp.int32))
    key_doc = jnp.concatenate([rim_doc, own_doc])[None, :]
    query_doc = own_doc[:, None]

    qkv_own = jnp.concatenate([w_query, w_key, w_value], axis=1)
    qkv_pair = swapped(qkv_own, "tensor", 1)
    out_pair = swapped(w_out, "tensor", 1)

    inputs = jnp.concatenate([rim[:, :width], hidden_in], axis=0).astype(jnp.float32)
    mean_square = jnp.mean(inputs * inputs, axis=1, keepdims=True)
    normed = (inputs * lax.rsqrt(mean_square + eps) * norm_gain[None, :]).astype(jnp.bfloat16)
    extended = normed.astype(jnp.float32)
    held = rows + WINDOW
    begin = lead - WINDOW
    convolved = jnp.zeros((held, width), jnp.float32)
    for tap in range(taps):
        convolved = convolved + conv_weight[tap][None, :] * extended[begin - tap : begin - tap + held]
    mixed = convolved.astype(jnp.bfloat16)

    cosine, sine = tables(held, line * rows - WINDOW)

    def attended(proj):
        return attention(proj, cosine, sine, query_doc, key_doc, query_cols, key_cols)

    near = jnp.zeros((rows, width), jnp.float32)
    for weights, outs in ((qkv_own, w_out), (qkv_pair, out_pair)):
        near = near + product(attended(product(mixed, weights)), outs)

    mixed_slots = [
        lax.dynamic_slice_in_dim(mixed, (place ^ k) * quarter, quarter, 1) for k in range(4)
    ]
    qkv_cross = [swapped(piece, "tensor", 1) for piece in qkv_far]
    out_cross = [swapped(piece, "tensor", 1) for piece in out_far]
    total = near + hidden_in.astype(jnp.float32)
    for slots, outs in ((qkv_far, out_far), (qkv_cross, out_cross)):
        proj = product(mixed_slots[0], slots[0])
        for k in range(1, 4):
            proj = proj + product(mixed_slots[k], slots[k])
        seen = attended(proj)
        ordered = jnp.concatenate(
            [
                lax.dynamic_slice_in_dim(seen, (place ^ k) * out_quarter, out_quarter, 1)
                for k in range(4)
            ],
            axis=1,
        )
        total = total + product(ordered, jnp.concatenate(outs, axis=0))
    return total.astype(jnp.bfloat16)


def solution(mesh):
    in_specs = (
        P(("dp", "seq", "tensor"), None),
        P(),
        P(),
        P(None, "tensor"),
        P(None, "tensor"),
        P(None, "tensor"),
        P("tensor", None),
        P(("dp", "seq")),
    )
    out_specs = P(("dp", "seq", "tensor"), None)
    return jax.shard_map(local, mesh=mesh, in_specs=in_specs, out_specs=out_specs, check_vma=False)
```

```python
import math

import jax
import jax.numpy as jnp
from jax import lax
from jax.experimental import pallas as pl
from jax.experimental.pallas import tpu as pltpu
from jax.sharding import PartitionSpec as P

HEAD = 64
WINDOW = 128
LANES = 128

eps = 1e-05
rope_base = 150000.0


def swapped(array, axis, bit):
    devices = lax.axis_size(axis)
    return lax.ppermute(array, axis, [(i, i ^ bit) for i in range(devices)])


def tables(rows, start):
    half = HEAD // 2
    frequency = jnp.exp(jnp.arange(half, dtype=jnp.float32) * (-2.0 * math.log(rope_base) / HEAD))
    positions = start + jnp.arange(rows, dtype=jnp.int32)
    angle = frequency[:, None] * positions.astype(jnp.float32)[None, :]
    return jnp.cos(angle), jnp.sin(angle)


def mixing_kernel(rim, hidden, gain, taps, out, normed):
    lead, width = rim.shape
    rows = hidden.shape[0]
    step = 16

    def scaled(values, at):
        values = values.astype(jnp.float32)
        mean_square = jnp.mean(values * values, axis=1, keepdims=True)
        done = values * lax.rsqrt(mean_square + eps) * gain[:, :]
        normed[pl.ds(at, step), :] = done.astype(jnp.bfloat16).astype(jnp.float32)

    def from_rim(i, carry):
        at = pl.multiple_of(i * step, step)
        scaled(rim[pl.ds(at, step), :], at)
        return carry

    def from_hidden(i, carry):
        at = pl.multiple_of(i * step, step)
        scaled(hidden[pl.ds(at, step), :], pl.multiple_of(lead + at, step))
        return carry

    lax.fori_loop(0, lead // step, from_rim, 0)
    lax.fori_loop(0, rows // step, from_hidden, 0)
    begin = lead - WINDOW

    def convolve(i, carry):
        at = pl.multiple_of(i * step, step)
        for left in range(0, width, 512):
            right = min(left + 512, width)
            held = normed[pl.ds(pl.multiple_of(at + begin - 8, 8), step + 8), left:right]
            total = taps[0:1, left:right] * held[8:]
            for tap in range(1, taps.shape[0]):
                total = total + taps[tap : tap + 1, left:right] * held[8 - tap : 8 - tap + step]
            out[pl.ds(at, step), left:right] = total.astype(jnp.bfloat16)
        return carry

    lax.fori_loop(0, out.shape[0] // step, convolve, 0)


def mixing(rim, hidden, gain, taps):
    lead, width = rim.shape
    rows = hidden.shape[0]
    return pl.pallas_call(
        mixing_kernel,
        out_shape=jax.ShapeDtypeStruct((rows + WINDOW, width), jnp.bfloat16),
        scratch_shapes=[pltpu.VMEM((rows + lead, width), jnp.float32)],
        cost_estimate=pl.CostEstimate(
            flops=rows * width * 200, bytes_accessed=rows * width * 4, transcendentals=rows
        ),
        name="mixing",
    )(rim, hidden, gain[None, :], taps)


def attention_kernel(query_cols, key_cols, proj, cosine, sine, query_doc, key_doc, out, qs, ks, vs):
    span = out.shape[0]
    half = HEAD // 2
    groups = query_cols // key_cols
    cos = cosine[:, :]
    sin = sine[:, :]

    def turned(at):
        flat = proj[:, at : at + LANES].T
        parts = []
        for h in range(LANES // HEAD):
            a = flat[h * HEAD : h * HEAD + half]
            b = flat[h * HEAD + half : (h + 1) * HEAD]
            parts += [a * cos - b * sin, b * cos + a * sin]
        return jnp.concatenate(parts, axis=0)

    for at in range(0, query_cols, LANES):
        qs[at : at + LANES, :] = (turned(at) * (1.0 / math.sqrt(HEAD))).astype(jnp.bfloat16)
    for at in range(0, key_cols, LANES):
        ks[:, at : at + LANES] = turned(query_cols + at).T.astype(jnp.bfloat16)
        first = query_cols + key_cols + at
        vs[at : at + LANES, :] = proj[:, first : first + LANES].T.astype(jnp.bfloat16)
    row = lax.broadcasted_iota(jnp.int32, (2 * WINDOW, WINDOW), 0)
    col = lax.broadcasted_iota(jnp.int32, (2 * WINDOW, WINDOW), 1)
    band = (row > col) & (row <= col + WINDOW)

    def block(i, carry):
        q0 = pl.multiple_of(i * WINDOW, WINDOW)
        held = pl.ds(q0, 2 * WINDOW)
        asking = pl.ds(pl.multiple_of(q0 + WINDOW, WINDOW), WINDOW)
        same = key_doc[held, :] == query_doc[:, pl.ds(q0, WINDOW)]
        bias = jnp.where(band & same, 0.0, -1e30)
        bias = jnp.concatenate([bias] * groups, axis=1)
        for kv in range(key_cols // HEAD):
            stacked = jnp.concatenate(
                [
                    qs[(kv * groups + g) * HEAD : (kv * groups + g + 1) * HEAD, asking]
                    for g in range(groups)
                ],
                axis=1,
            )
            key = ks[held, kv * HEAD : (kv + 1) * HEAD]
            value = vs[kv * HEAD : (kv + 1) * HEAD, held]
            scores = jnp.dot(key, stacked, preferred_element_type=jnp.float32) + bias
            largest = jnp.max(scores, axis=0, keepdims=True)
            weights = jnp.exp(scores - largest)
            total = jnp.sum(weights, axis=0, keepdims=True)
            summed = jnp.dot(value, weights.astype(jnp.bfloat16), preferred_element_type=jnp.float32)
            result = summed / total
            per = LANES // HEAD
            for g in range(0, groups, per):
                pair = jnp.concatenate(
                    [result[:, (g + h) * WINDOW : (g + h + 1) * WINDOW] for h in range(per)], axis=0
                )
                at = (kv * groups + g) * HEAD
                out[pl.ds(q0, WINDOW), at : at + LANES] = pair.T.astype(jnp.bfloat16)
        return carry

    lax.fori_loop(0, span // WINDOW, block, 0)


def attention(proj, cosine, sine, query_doc, key_doc, query_cols, key_cols):
    rows = query_doc.shape[1]
    held = proj.shape[0]

    def kernel(*refs):
        attention_kernel(query_cols, key_cols, *refs)

    return pl.pallas_call(
        kernel,
        out_shape=jax.ShapeDtypeStruct((rows, query_cols), jnp.bfloat16),
        scratch_shapes=[
            pltpu.VMEM((query_cols, held), jnp.bfloat16),
            pltpu.VMEM((held, key_cols), jnp.bfloat16),
            pltpu.VMEM((key_cols, held), jnp.bfloat16),
        ],
        cost_estimate=pl.CostEstimate(
            flops=rows * query_cols * 2 * WINDOW * 4,
            bytes_accessed=proj.size * 4,
            transcendentals=rows * query_cols // HEAD * 2 * WINDOW,
        ),
        name="attention",
    )(proj, cosine, sine, query_doc, key_doc)


def product(left, right):
    return jnp.dot(left, right, preferred_element_type=jnp.float32)


def local(hidden_in, norm_gain, conv_weight, w_query, w_key, w_value, w_out, doc_ids):
    rows, width = hidden_in.shape
    taps = conv_weight.shape[0]
    query_cols = w_query.shape[1]
    key_cols = w_key.shape[1]
    tensors = lax.axis_size("tensor")
    part = lax.axis_index("tensor")
    line = lax.axis_index("seq") * tensors + part
    far = tensors // 2
    place = 2 * (lax.axis_index("seq") % 2) + lax.axis_index("dp") % 2
    quarter = width // 4
    out_quarter = query_cols // 4

    def qkv_piece(which):
        at = which * quarter
        return jnp.concatenate(
            [lax.dynamic_slice_in_dim(w, at, quarter, 0) for w in (w_query, w_key, w_value)], axis=1
        )

    def out_piece(which):
        return lax.dynamic_slice_in_dim(w_out, which * out_quarter, out_quarter, 0)

    barrier = lax.optimization_barrier
    core = 1

    lead = WINDOW + 16
    own_doc = lax.dynamic_slice_in_dim(doc_ids, part * rows, rows, 0)
    sent = jnp.concatenate(
        [
            hidden_in[rows - lead :],
            jnp.broadcast_to(
                own_doc[rows - lead :].astype(jnp.bfloat16)[:, None], (lead, LANES)
            ),
        ],
        axis=1,
    )
    devices = lax.axis_size("seq") * tensors
    rim = lax.ppermute(sent, ("seq", "tensor"), [(i, i + 1) for i in range(devices - 1)])

    qkv_zero = swapped(qkv_piece(place), "tensor", far)
    qkv_own = jnp.concatenate([w_query, w_key, w_value], axis=1)
    qkv_pair = swapped(qkv_own, "tensor", core)
    out_pair = swapped(w_out, "tensor", core)

    rim_doc = jnp.where(line == 0, -1, rim[lead - WINDOW :, width].astype(jnp.int32))
    key_doc = jnp.concatenate([rim_doc, own_doc])[:, None]
    query_doc = own_doc[None, :]
    held = rows + WINDOW
    cosine, sine = tables(held, line * rows - WINDOW)
    mixed = mixing(rim[:, :width], hidden_in, norm_gain, conv_weight)

    def attended(proj):
        return attention(proj, cosine, sine, query_doc, key_doc, query_cols, key_cols)

    def ordered(seen):
        return jnp.concatenate(
            [
                lax.dynamic_slice_in_dim(seen, (place ^ k) * out_quarter, out_quarter, 1)
                for k in range(4)
            ],
            axis=1,
        )

    proj = product(mixed, qkv_own)
    proj, qkv_zero, last = barrier((proj, qkv_zero, qkv_piece(place ^ 3)))

    qkv_three = swapped(last, "tensor", far)
    qkv_one = swapped(qkv_zero, "dp", 1)
    qkv_two = swapped(qkv_zero, "seq", 1)
    qkv_zero_cross = swapped(qkv_zero, "tensor", core)
    total = hidden_in.astype(jnp.float32) + product(attended(proj), w_out)
    total, qkv_pair, out_pair = barrier((total, qkv_pair, out_pair))
    pair_seen = attended(product(mixed, qkv_pair))
    mixed_slots = jnp.concatenate(
        [lax.dynamic_slice_in_dim(mixed, (place ^ k) * quarter, quarter, 1) for k in range(4)],
        axis=1,
    )
    pair_seen, mixed_slots, qkv_one, qkv_two, qkv_three, piece, last = barrier(
        (pair_seen, mixed_slots, qkv_one, qkv_two, qkv_three, out_piece(place), out_piece(place ^ 3))
    )

    out_zero = swapped(piece, "tensor", far)
    cross = [swapped(a, "tensor", core) for a in (qkv_one, qkv_two, qkv_three)]
    total = total + product(pair_seen, out_pair)
    qkv_far = jnp.concatenate([qkv_zero, qkv_one, qkv_two, qkv_three], axis=0)
    far_seen = ordered(attended(product(mixed_slots, qkv_far)))
    far_seen, out_zero, last, total = barrier((far_seen, out_zero, last, total))

    out_three = swapped(last, "tensor", far)
    out_one = swapped(out_zero, "dp", 1)
    out_two = swapped(out_zero, "seq", 1)
    out_zero_cross = swapped(out_zero, "tensor", core)
    qkv_cross = jnp.concatenate([qkv_zero_cross] + cross, axis=0)
    cross_seen = ordered(attended(product(mixed_slots, qkv_cross)))
    cross_seen, out_one, out_two, out_three = barrier((cross_seen, out_one, out_two, out_three))

    cross = [swapped(a, "tensor", core) for a in (out_one, out_two, out_three)]
    far_out = jnp.concatenate([out_zero, out_one, out_two, out_three], axis=0)
    total = total + product(far_seen, far_out)
    cross_out = jnp.concatenate([out_zero_cross] + cross, axis=0)
    total = total + product(cross_seen, cross_out)
    return total.astype(jnp.bfloat16)


def solution(mesh):
    in_specs = (
        P(("dp", "seq", "tensor"), None),
        P(),
        P(),
        P(None, "tensor"),
        P(None, "tensor"),
        P(None, "tensor"),
        P("tensor", None),
        P(("dp", "seq")),
    )
    out_specs = P(("dp", "seq", "tensor"), None)
    return jax.shard_map(local, mesh=mesh, in_specs=in_specs, out_specs=out_specs, check_vma=False)
```

```python
import math

import jax
import jax.numpy as jnp
from jax import lax
from jax.experimental import pallas as pl
from jax.experimental.pallas import tpu as pltpu
from jax.sharding import PartitionSpec as P

HEAD = 64
WINDOW = 128
LANES = 128

eps = 1e-05
rope_base = 150000.0


def swapped(array, axis, bit):
    devices = lax.axis_size(axis)
    return lax.ppermute(array, axis, [(i, i ^ bit) for i in range(devices)])


def tables(rows, start):
    half = HEAD // 2
    frequency = jnp.exp(jnp.arange(half, dtype=jnp.float32) * (-2.0 * math.log(rope_base) / HEAD))
    positions = start + jnp.arange(rows, dtype=jnp.int32)
    angle = frequency[:, None] * positions.astype(jnp.float32)[None, :]
    return jnp.cos(angle), jnp.sin(angle)


def mixing_kernel(rim, hidden, gain, taps, out, normed):
    lead, width = rim.shape
    rows = hidden.shape[0]
    step = 16

    def scaled(values, at):
        values = values.astype(jnp.float32)
        mean_square = jnp.mean(values * values, axis=1, keepdims=True)
        done = values * lax.rsqrt(mean_square + eps) * gain[:, :]
        normed[pl.ds(at, step), :] = done.astype(jnp.bfloat16).astype(jnp.float32)

    def from_rim(i, carry):
        at = pl.multiple_of(i * step, step)
        scaled(rim[pl.ds(at, step), :], at)
        return carry

    def from_hidden(i, carry):
        at = pl.multiple_of(i * step, step)
        scaled(hidden[pl.ds(at, step), :], pl.multiple_of(lead + at, step))
        return carry

    lax.fori_loop(0, lead // step, from_rim, 0)
    lax.fori_loop(0, rows // step, from_hidden, 0, unroll=2)
    begin = lead - WINDOW

    def convolve(i, carry):
        at = pl.multiple_of(i * step, step)
        for left in range(0, width, 512):
            right = min(left + 512, width)
            held = normed[pl.ds(pl.multiple_of(at + begin - 8, 8), step + 8), left:right]
            total = taps[0:1, left:right] * held[8:]
            for tap in range(1, taps.shape[0]):
                total = total + taps[tap : tap + 1, left:right] * held[8 - tap : 8 - tap + step]
            out[pl.ds(at, step), left:right] = total.astype(jnp.bfloat16)
        return carry

    lax.fori_loop(0, out.shape[0] // step, convolve, 0, unroll=2)


def mixing(rim, hidden, gain, taps):
    lead, width = rim.shape
    rows = hidden.shape[0]
    return pl.pallas_call(
        mixing_kernel,
        out_shape=jax.ShapeDtypeStruct((rows + WINDOW, width), jnp.bfloat16),
        scratch_shapes=[pltpu.VMEM((rows + lead, width), jnp.float32)],
        cost_estimate=pl.CostEstimate(
            flops=rows * width * 200, bytes_accessed=rows * width * 4, transcendentals=rows
        ),
        name="mixing",
    )(rim, hidden, gain[None, :], taps)


def attention_kernel(query_cols, key_cols, mixed, weights, rest):
    cosine, sine, query_doc, key_doc, out, proj, qs, ks, vs = rest
    span = out.shape[0]
    for k, held in enumerate(mixed):
        left = 0
        for part in weights[k]:
            for at in range(0, part.shape[1], 2 * LANES):
                size = min(2 * LANES, part.shape[1] - at)
                piece = jnp.dot(
                    held[:, :], part[:, at : at + size], preferred_element_type=jnp.float32
                )
                if k == 0:
                    proj[:, left + at : left + at + size] = piece
                else:
                    proj[:, left + at : left + at + size] += piece
            left += part.shape[1]
    half = HEAD // 2
    groups = query_cols // key_cols
    cos = cosine[:, :]
    sin = sine[:, :]

    def turned(at):
        flat = proj[:, at : at + LANES].T
        parts = []
        for h in range(LANES // HEAD):
            a = flat[h * HEAD : h * HEAD + half]
            b = flat[h * HEAD + half : (h + 1) * HEAD]
            parts += [a * cos - b * sin, b * cos + a * sin]
        return jnp.concatenate(parts, axis=0)

    for at in range(0, query_cols, LANES):
        qs[at : at + LANES, :] = (turned(at) * (1.0 / math.sqrt(HEAD))).astype(jnp.bfloat16)
    for at in range(0, key_cols, LANES):
        ks[:, at : at + LANES] = turned(query_cols + at).T.astype(jnp.bfloat16)
        first = query_cols + key_cols + at
        vs[at : at + LANES, :] = proj[:, first : first + LANES].T.astype(jnp.bfloat16)
    row = lax.broadcasted_iota(jnp.int32, (2 * WINDOW, WINDOW), 0)
    col = lax.broadcasted_iota(jnp.int32, (2 * WINDOW, WINDOW), 1)
    band = (row > col) & (row <= col + WINDOW)

    def block(i, carry):
        q0 = pl.multiple_of(i * WINDOW, WINDOW)
        held = pl.ds(q0, 2 * WINDOW)
        asking = pl.ds(pl.multiple_of(q0 + WINDOW, WINDOW), WINDOW)
        same = key_doc[held, :] == query_doc[:, pl.ds(q0, WINDOW)]
        bias = jnp.where(band & same, 0.0, -1e30)
        bias = jnp.concatenate([bias] * groups, axis=1)
        for kv in range(key_cols // HEAD):
            stacked = jnp.concatenate(
                [
                    qs[(kv * groups + g) * HEAD : (kv * groups + g + 1) * HEAD, asking]
                    for g in range(groups)
                ],
                axis=1,
            )
            key = ks[held, kv * HEAD : (kv + 1) * HEAD]
            value = vs[kv * HEAD : (kv + 1) * HEAD, held]
            scores = jnp.dot(key, stacked, preferred_element_type=jnp.float32) + bias
            largest = jnp.max(scores, axis=0, keepdims=True)
            weights = jnp.exp(scores - largest)
            total = jnp.sum(weights, axis=0, keepdims=True)
            summed = jnp.dot(value, weights.astype(jnp.bfloat16), preferred_element_type=jnp.float32)
            result = summed / total
            per = LANES // HEAD
            for g in range(0, groups, per):
                pair = jnp.concatenate(
                    [result[:, (g + h) * WINDOW : (g + h + 1) * WINDOW] for h in range(per)], axis=0
                )
                at = (kv * groups + g) * HEAD
                out[pl.ds(q0, WINDOW), at : at + LANES] = pair.T.astype(jnp.bfloat16)
        return carry

    lax.fori_loop(0, span // WINDOW, block, 0)


def attention(mixed, weights, cosine, sine, query_doc, key_doc, query_cols, key_cols):
    rows = query_doc.shape[1]
    held = mixed[0].shape[0]
    counts = [len(parts) for parts in weights]
    flat = [part for parts in weights for part in parts]

    def kernel(*refs):
        refs = list(refs)
        left = [refs.pop(0) for _ in mixed]
        right = [[refs.pop(0) for _ in range(count)] for count in counts]
        attention_kernel(query_cols, key_cols, left, right, refs)

    columns = query_cols + 2 * key_cols
    return pl.pallas_call(
        kernel,
        out_shape=jax.ShapeDtypeStruct((rows, query_cols), jnp.bfloat16),
        scratch_shapes=[
            pltpu.VMEM((held, columns), jnp.float32),
            pltpu.VMEM((query_cols, held), jnp.bfloat16),
            pltpu.VMEM((held, key_cols), jnp.bfloat16),
            pltpu.VMEM((key_cols, held), jnp.bfloat16),
        ],
        cost_estimate=pl.CostEstimate(
            flops=2 * held * columns * sum(m.shape[1] for m in mixed),
            bytes_accessed=sum(2 * a.size for a in [*mixed, *flat]),
            transcendentals=rows * query_cols // HEAD * 2 * WINDOW,
        ),
        name="attention",
    )(*mixed, *flat, cosine, sine, query_doc, key_doc)


def product(left, right):
    return jnp.dot(left, right, preferred_element_type=jnp.float32)


def local(hidden_in, norm_gain, conv_weight, w_query, w_key, w_value, w_out, doc_ids):
    rows, width = hidden_in.shape
    taps = conv_weight.shape[0]
    query_cols = w_query.shape[1]
    key_cols = w_key.shape[1]
    tensors = lax.axis_size("tensor")
    part = lax.axis_index("tensor")
    line = lax.axis_index("seq") * tensors + part
    far = tensors // 2
    place = 2 * (lax.axis_index("seq") % 2) + lax.axis_index("dp") % 2
    quarter = width // 4
    out_quarter = query_cols // 4

    def qkv_piece(which):
        at = which * quarter
        return jnp.concatenate(
            [lax.dynamic_slice_in_dim(w, at, quarter, 0) for w in (w_query, w_key, w_value)], axis=1
        )

    def out_piece(which):
        return lax.dynamic_slice_in_dim(w_out, which * out_quarter, out_quarter, 0)

    barrier = lax.optimization_barrier
    core = 1

    lead = WINDOW + 16
    own_doc = lax.dynamic_slice_in_dim(doc_ids, part * rows, rows, 0)
    sent = jnp.concatenate(
        [
            hidden_in[rows - lead :],
            jnp.broadcast_to(
                own_doc[rows - lead :].astype(jnp.bfloat16)[:, None], (lead, LANES)
            ),
        ],
        axis=1,
    )
    devices = lax.axis_size("seq") * tensors
    rim = lax.ppermute(sent, ("seq", "tensor"), [(i, i + 1) for i in range(devices - 1)])

    qkv_zero = swapped(qkv_piece(place), "tensor", far)
    qkv_own = (w_query, w_key, w_value)
    qkv_pair = tuple(swapped(w, "tensor", core) for w in qkv_own)
    out_pair = swapped(w_out, "tensor", core)

    rim_doc = jnp.where(line == 0, -1, rim[lead - WINDOW :, width].astype(jnp.int32))
    key_doc = jnp.concatenate([rim_doc, own_doc])[:, None]
    query_doc = own_doc[None, :]
    held = rows + WINDOW
    cosine, sine = tables(held, line * rows - WINDOW)
    mixed = mixing(rim[:, :width], hidden_in, norm_gain, conv_weight)

    def attended(left, weights):
        return attention(left, weights, cosine, sine, query_doc, key_doc, query_cols, key_cols)

    def ordered(seen):
        return jnp.concatenate(
            [
                lax.dynamic_slice_in_dim(seen, (place ^ k) * out_quarter, out_quarter, 1)
                for k in range(4)
            ],
            axis=1,
        )

    own_seen = attended([mixed], [qkv_own])
    own_seen, qkv_zero, last = barrier((own_seen, qkv_zero, qkv_piece(place ^ 3)))

    qkv_three = swapped(last, "tensor", far)
    qkv_one = swapped(qkv_zero, "dp", 1)
    qkv_two = swapped(qkv_zero, "seq", 1)
    qkv_zero_cross = swapped(qkv_zero, "tensor", core)
    total = hidden_in.astype(jnp.float32) + product(own_seen, w_out)
    total, qkv_pair, out_pair = barrier((total, qkv_pair, out_pair))
    pair_seen = attended([mixed], [qkv_pair])
    mixed_slots = [
        lax.dynamic_slice_in_dim(mixed, (place ^ k) * quarter, quarter, 1) for k in range(4)
    ]
    pair_seen, mixed_slots, qkv_one, qkv_two, qkv_three, piece, last = barrier(
        (pair_seen, mixed_slots, qkv_one, qkv_two, qkv_three, out_piece(place), out_piece(place ^ 3))
    )

    out_zero = swapped(piece, "tensor", far)
    cross = [swapped(a, "tensor", core) for a in (qkv_one, qkv_two, qkv_three)]
    qkv_far = [[qkv_zero], [qkv_one], [qkv_two], [qkv_three]]
    far_seen = ordered(attended(mixed_slots, qkv_far))
    total = total + product(pair_seen, out_pair)
    far_seen, out_zero, last, total = barrier((far_seen, out_zero, last, total))

    out_three = swapped(last, "tensor", far)
    out_one = swapped(out_zero, "dp", 1)
    out_two = swapped(out_zero, "seq", 1)
    out_zero_cross = swapped(out_zero, "tensor", core)
    qkv_cross = [[a] for a in [qkv_zero_cross] + cross]
    cross_seen = ordered(attended(mixed_slots, qkv_cross))
    cross_seen, out_one, out_two, out_three = barrier((cross_seen, out_one, out_two, out_three))

    cross = [swapped(a, "tensor", core) for a in (out_one, out_two, out_three)]
    far_out = jnp.concatenate([out_zero, out_one, out_two, out_three], axis=0)
    total = total + product(far_seen, far_out)
    cross_out = jnp.concatenate([out_zero_cross] + cross, axis=0)
    total = total + product(cross_seen, cross_out)
    return total.astype(jnp.bfloat16)


def solution(mesh):
    in_specs = (
        P(("dp", "seq", "tensor"), None),
        P(),
        P(),
        P(None, "tensor"),
        P(None, "tensor"),
        P(None, "tensor"),
        P("tensor", None),
        P(("dp", "seq")),
    )
    out_specs = P(("dp", "seq", "tensor"), None)
    return jax.shard_map(local, mesh=mesh, in_specs=in_specs, out_specs=out_specs, check_vma=False)
```
